32 devices in a mesh: group: 8 (over z, y), rep: 4 (over x, core).
Axes of the slice: x: 2, y: 2, z: 4, core: 2. Of those that a mesh axis runs over, the one named last changes fastest.
Arguments:
- grad_parts: bfloat16 [4, 24, 1024, 1024], P('rep', None, 'group'), may hold values from -40 to 40
- params: bfloat16 [24, 1024, 1024], P('rep', 'group'), may hold values from -6 to 6
- accum: float32 [24, 1024, 1024], P('rep', 'group'), may hold values from 1 to 50
- left_pre: bfloat16 [4, 8, 1, 1024, 1024], P('rep', 'group'), may hold values from -1 to 4
- right_pre: bfloat16 [4, 8, 1, 1024, 1024], P('rep', 'group'), may hold values from -1 to 4
- slot_block: int32 [4, 8, 1], replicated, may hold values from -1 to 5, as said below
- layer_of: int32 [24], replicated, may hold values from 0 to 7
Outputs:
- new_params: bfloat16 [24, 1024, 1024], P(None, 'group')
- new_accum: float32 [24, 1024, 1024], P('rep', 'group')
The draws below stay inside these ranges and needn't reach their ends.
Inputs may be any that keep to these rules, and one draw needn't show every extreme that they name: For every replica q each of its 6 blocks is named by exactly one slot of slot_block[q]; a device's used slots come first and the others hold -1; in every replica some device has all 1 slots used.
All inputs are finite; a program needn't handle non-finite values.
Results may differ from the reference program's by a relative error of at most 0.018.
Values may be sent and summed in bfloat16 or wider, within the bound.
A program may use at most 128 MiB of HBM per device.

```python
import math
import jax
import jax.numpy as jnp
from jax import lax

B = 1024
SLOTS = 1
LAYERS = 8
RB = 6
NB = 24
N_GROUP = 8
N_REP = 4


def draw_grad_parts(key, part):
    key_noise, key_cols, key_blocks = jax.random.split(jax.random.fold_in(key, 11), 3)
    full_shape = (N_REP, NB, B, B)
    row_place = jnp.arange(B, dtype=jnp.float32) / (B - 1)
    col_scale = 10.0 ** (jax.random.uniform(key_cols, (B,), jnp.float32) - 0.5)
    block_scale = jnp.exp(jax.random.uniform(key_blocks, (NB,), jnp.float32, -1.6, 1.6))
    pattern = jax.random.normal(key_noise, full_shape, jnp.float32)
    row_scale = 10.0 ** (row_place - 0.5)
    drawn = pattern * row_scale[:, None] * col_scale[None, :] * block_scale[:, None, None]
    return jnp.clip(drawn, -40.0, 40.0).astype(jnp.bfloat16)


def precond_matrices(key, salt):
    key_noise, key_diagonal = jax.random.split(jax.random.fold_in(key, salt))
    full_shape = (N_REP, N_GROUP, SLOTS, B, B)
    noise = jnp.clip(jax.random.normal(key_noise, full_shape, jnp.float32), -6.0, 6.0)
    symmetric = (noise + jnp.swapaxes(noise, -1, -2)) * (0.45 / math.sqrt(2.0 * B))
    diagonal = jnp.exp(jax.random.uniform(key_diagonal, full_shape[:-1], jnp.float32, math.log(1.2), math.log(4.0)))
    on_diagonal = jnp.arange(B)[:, None] == jnp.arange(B)[None, :]
    return jnp.where(on_diagonal, diagonal[..., :, None], symmetric).astype(jnp.bfloat16)


def draw_left_pre(key, part):
    return precond_matrices(key, 21)


def draw_right_pre(key, part):
    return precond_matrices(key, 37)


def replica_table(replica_key):
    key_order, key_blocks = jax.random.split(replica_key, 2)
    device_order = jax.random.permutation(key_order, N_GROUP)
    device_rank = jnp.arange(N_GROUP, dtype=jnp.int32)
    owned = device_rank < RB
    block_order = jax.random.permutation(key_blocks, RB)
    block_position = jnp.clip(device_rank, 0, RB - 1)
    entries = jnp.where(owned, block_order[block_position], -1)[:, None]
    inverse = jnp.argsort(device_order, stable=True)
    return entries[inverse]


def draw_slot_block(key, part):
    replica_keys = jax.random.split(jax.random.fold_in(key, 5), N_REP)
    return jax.vmap(replica_table)(replica_keys).astype(jnp.int32)


def place_ends(array, stream_key, least, top_value):
    place = [jax.random.randint(jax.random.fold_in(stream_key, axis), (), 0, length) for axis, length in enumerate(array.shape)]
    longest = array.shape.index(max(array.shape))
    next_to = place[:longest] + [(place[longest] + 1) % array.shape[longest]] + place[longest + 1:]
    return array.at[tuple(place)].set(least).at[tuple(next_to)].set(top_value)


def shard_levels(own_key, extent, pieces, smallest, largest):
    def one(dim, blocks):
        draws = jax.random.uniform(jax.random.fold_in(jax.random.fold_in(own_key, 6), dim), (blocks,), jnp.float32, smallest / len(pieces), largest / len(pieces))
        return jnp.repeat(jnp.exp(draws), extent[dim] // blocks).reshape((-1,) + (1,) * (len(extent) - dim - 1))

    factor_of = one(*pieces[0])
    for cut in pieces[1:]:
        factor_of = factor_of * one(*cut)
    return factor_of


def bell_draw(key, shape, spread, bound, cuts=(), kind=jnp.bfloat16):
    array = spread * jax.random.normal(key, shape, jnp.float32)
    if cuts:
        array = array * shard_levels(key, shape, cuts, -0.22, 0.18)
    return jnp.clip(array, -bound, bound).astype(kind)


def setup_inputs(seed: int = 0) -> dict:
    streams_of = jax.random.split(jax.random.key(seed), 8)
    return {
        "grad_parts": draw_grad_parts(jax.random.fold_in(streams_of[7], 71), 0),
        "params": bell_draw(streams_of[1], (NB, B, B), 1.0, 6.0, ((0, 4), (1, 8))),
        "accum": jnp.clip(jnp.exp(math.log(50.0) - 3.912023 * jax.random.uniform(streams_of[2], (NB, B, B), jnp.float32) ** shard_levels(streams_of[2], (NB, B, B), ((0, 4), (1, 8)), -0.2, 0.2)), 1.0, 50.0),
        "left_pre": draw_left_pre(jax.random.fold_in(streams_of[7], 71), 0),
        "right_pre": draw_right_pre(jax.random.fold_in(streams_of[7], 71), 0),
        "slot_block": draw_slot_block(jax.random.fold_in(streams_of[7], 71), 0),
        "layer_of": place_ends(jax.random.randint(streams_of[6], (NB,), 0, LAYERS), jax.random.fold_in(streams_of[6], 1), 0, LAYERS - 1).astype(jnp.int32),
    }


step_rate = 0.5

def reference(grad_parts, params, accum, left_pre, right_pre, slot_block, layer_of):
    summed = jnp.zeros(grad_parts.shape[1:], jnp.float32)
    for replica in range(N_REP):
        summed = summed + grad_parts[replica].astype(jnp.float32)
    gradient = summed.astype(jnp.bfloat16)
    gradient_wide = gradient.astype(jnp.float32)
    new_accum = accum + gradient_wide * gradient_wide
    graft = gradient_wide * lax.rsqrt(new_accum)
    graft_blocks = lax.optimization_barrier(jnp.sum(graft * graft, axis=(1, 2)))
    flat_table = slot_block.reshape(-1)
    slot_total = flat_table.shape[0]
    owner_replica = jnp.arange(slot_total, dtype=jnp.int32) // (N_GROUP * SLOTS)
    global_block = jnp.where(flat_table >= 0, owner_replica * RB + flat_table, -1)
    position = lax.optimization_barrier(jnp.sum(jnp.where(global_block[None, :] == jnp.arange(NB, dtype=jnp.int32)[:, None], jnp.arange(slot_total, dtype=jnp.int32)[None, :], 0), axis=1)).astype(jnp.int32)
    lefts = left_pre.reshape(slot_total, B, B)
    rights = right_pre.reshape(slot_total, B, B)

    def one_block(block_index):
        slot_index = position[block_index]
        left_product = jnp.dot(lefts[slot_index], gradient[block_index], preferred_element_type=jnp.float32).astype(jnp.bfloat16)
        return jnp.dot(left_product, rights[slot_index], preferred_element_type=jnp.float32).astype(jnp.bfloat16)
    precond = lax.map(one_block, jnp.arange(NB, dtype=jnp.int32))
    precond_wide = precond.astype(jnp.float32)
    shampoo_blocks = lax.optimization_barrier(jnp.sum(precond_wide * precond_wide, axis=(1, 2)))
    onehot = (layer_of[:, None] == jnp.arange(LAYERS, dtype=jnp.int32)[None, :]).astype(jnp.float32)
    graft_sq = lax.optimization_barrier(jnp.sum(onehot * graft_blocks[:, None], axis=0))
    shampoo_sq = lax.optimization_barrier(jnp.sum(onehot * shampoo_blocks[:, None], axis=0))
    layer_scale = jnp.sqrt(graft_sq) * lax.rsqrt(shampoo_sq + 1e-06)
    block_scale = lax.optimization_barrier(jnp.sum(onehot * layer_scale[None, :], axis=1))
    new_params = (params.astype(jnp.float32) - step_rate * block_scale[:, None, None] * precond_wide).astype(jnp.bfloat16)
    return (new_params, new_accum)
```

```python
import functools

import jax
import jax.numpy as jnp
from jax import lax
from jax.experimental import pallas as pl
from jax.experimental.pallas import tpu as pltpu
from jax.sharding import PartitionSpec as P

MESH = pl.DeviceIdType.MESH
LAYERS = 8
LANES = 128
step_rate = 0.5
F32 = jnp.float32
BF16 = jnp.bfloat16


def kernel(
    n, chunks, width, rb, rows, size, tile,
    table, layer_of, grad, params, accum, left, right,
    new_params, new_accum,
    own, pair_in, half_out, half_in, summed, slot_out, block_in, lefts, rights, total, precond,
    rows_in, param_in, updated, other_in, acc, graft_sq, shampoo_sq, scales, stat_mine, stat_group, stat_rep,
    load_sem, pair_send, pair_recv, half_send, half_recv, slot_send, slot_recv, back_send, back_recv,
    stat_send, stat_recv, stat_rep_send, stat_rep_recv, other_send, other_recv, core_send, core_recv,
    store_sem,
):
    g = lax.axis_index("group")
    r = lax.axis_index("rep")
    pair = r + 1 - 2 * (r % 2)
    half = r + 2 - 4 * ((r // 2) % 2)
    pair_half = pair + 2 - 4 * ((pair // 2) % 2)

    def cols(c):
        return pl.ds(c * width, width)

    def blocks(q):
        return pl.ds(q * rb, rb)

    def peer(k):
        return (g + 1 + (n // 2 - 1 + k) % (n - 1)) % n

    def remote(src, dst, send, recv, where):
        return pltpu.make_async_remote_copy(
            src_ref=src, dst_ref=dst, send_sem=send, recv_sem=recv, device_id=where, device_id_type=MESH
        )

    def load_own(c, which):
        q = (r, half)[which]
        return pltpu.make_async_copy(grad.at[0, blocks(q), :, cols(c)], own.at[c, which], load_sem.at[which, c])

    def load_accum(c):
        return pltpu.make_async_copy(accum.at[:, :, cols(c)], acc.at[c], load_sem.at[2, c])

    def load_param(c):
        return pltpu.make_async_copy(params.at[:, :, cols(c)], param_in.at[c], load_sem.at[3, c])

    load_left = pltpu.make_async_copy(left.at[0, 0, 0], lefts, load_sem.at[4, 0])
    load_right = pltpu.make_async_copy(right.at[0, 0, 0], rights, load_sem.at[4, 1])

    def store_accum(c):
        return pltpu.make_async_copy(acc.at[c], new_accum.at[:, :, cols(c)], store_sem.at[0, c])

    def send_pair(c, which):
        q = (pair, pair_half)[which]
        return remote(
            grad.at[0, blocks(q), :, cols(c)], pair_in.at[c, which],
            pair_send.at[c, which], pair_recv.at[c, which], {"rep": pair},
        )

    def send_half(c):
        return remote(half_out.at[c], half_in.at[c], half_send.at[c], half_recv.at[c], {"rep": half})

    def send_slot(c, d):
        return remote(
            slot_out.at[c, d], block_in.at[c, pl.ds(g * rows, rows), :],
            slot_send.at[c, d], slot_recv.at[c, g], {"group": d},
        )

    def recv_slot(c, d):
        return remote(
            slot_out.at[c, d], block_in.at[c, pl.ds(d * rows, rows), :],
            slot_send.at[c, d], slot_recv.at[c, d], {"group": d},
        )

    def send_back(c, d):
        return remote(
            precond.at[c, pl.ds(d * rows, rows), :], rows_in[c].at[g],
            back_send.at[c, d], back_recv.at[c, g], {"group": d},
        )

    def recv_back(c, d):
        return remote(
            precond.at[c, pl.ds(d * rows, rows), :], rows_in[c].at[d],
            back_send.at[c, d], back_recv.at[c, d], {"group": d},
        )

    def send_stat(d):
        return remote(stat_mine, stat_group.at[g], stat_send.at[d], stat_recv.at[g], {"group": d})

    def recv_stat(d):
        return remote(stat_mine, stat_group.at[d], stat_send.at[d], stat_recv.at[d], {"group": d})

    def send_stat_rep(i, where):
        return remote(
            stat_rep.at[2 * i], stat_rep.at[2 * i + 1], stat_rep_send.at[i], stat_rep_recv.at[i], {"rep": where}
        )

    def send_other(c):
        return remote(updated.at[c], other_in.at[c], other_send.at[c], other_recv.at[c], {"rep": half})

    def send_core(c, which):
        src = (updated, other_in)[which]
        q = (r, half)[which]
        return remote(
            src.at[c], new_params.at[blocks(q), :, cols(c)],
            core_send.at[c, which], core_recv.at[c, which], {"rep": pair},
        )

    def recv_core(c, which):
        src = (updated, other_in)[which]
        q = (pair, pair_half)[which]
        return remote(
            src.at[c], new_params.at[blocks(q), :, cols(c)],
            core_send.at[c, which], core_recv.at[c, which], {"rep": pair},
        )

    def store_param(c, which):
        src = (updated, other_in)[which]
        q = (r, half)[which]
        return pltpu.make_async_copy(src.at[c], new_params.at[blocks(q), :, cols(c)], store_sem.at[1 + which, c])

    def each_peer(act):
        def body(k, carry):
            act(peer(k))
            return carry

        lax.fori_loop(0, n - 1, body, 0)

    for c in range(chunks):
        load_own(c, 1).start()
        load_own(c, 0).start()

    barrier = pltpu.get_barrier_semaphore()
    each_peer(
        lambda d: pl.semaphore_signal(barrier, inc=1, device_id={"group": d}, device_id_type=MESH)
    )
    pl.semaphore_signal(barrier, inc=1, device_id={"rep": pair}, device_id_type=MESH)
    pl.semaphore_signal(barrier, inc=1, device_id={"rep": half}, device_id_type=MESH)
    pl.semaphore_wait(barrier, n + 1)

    for c in range(chunks):
        send_pair(c, 1).start()
        send_pair(c, 0).start()
    for c in range(chunks):
        load_accum(c).start()
    load_left.start()
    load_right.start()
    for c in range(chunks):
        load_param(c).start()

    graft_sq[...] = jnp.zeros_like(graft_sq)
    shampoo_sq[...] = jnp.zeros_like(shampoo_sq)

    for c in range(chunks):
        load_own(c, 1).wait()
        send_pair(c, 1).wait_recv()

        def add_pair(j, carry):
            half_out[c, j] = (own[c, 1, j].astype(F32) + pair_in[c, 1, j].astype(F32)).astype(BF16)
            return carry

        lax.fori_loop(0, rb, add_pair, 0)
        send_half(c).start()

    def sum_and_send(c):
        load_own(c, 0).wait()
        send_pair(c, 0).wait_recv()
        send_half(c).wait_recv()

        def add_half(j, carry):
            summed[c, j] = (
                own[c, 0, j].astype(F32) + pair_in[c, 0, j].astype(F32) + half_in[c, j].astype(F32)
            ).astype(BF16)
            return carry

        lax.fori_loop(0, rb, add_half, 0)

        def fill(d, carry):
            slot_out[c, d] = summed[c, jnp.maximum(table[r, d, 0], 0)]
            return carry

        lax.fori_loop(0, n, fill, 0)
        each_peer(lambda d: send_slot(c, d).start())
        block_in[c, pl.ds(g * rows, rows), :] = slot_out[c, g]

        load_accum(c).wait()

        def graft(j, carry):
            gradient = summed[c, j].astype(F32)
            now = acc[c, j] + gradient * gradient
            acc[c, j] = now
            scaled = gradient * lax.rsqrt(now)
            graft_sq[j] += jnp.sum((scaled * scaled).reshape(rows // 8, 8, width), axis=0)
            return carry

        lax.fori_loop(0, rb, graft, 0)
        store_accum(c).start()

    def multiply(c):
        each_peer(lambda d: recv_slot(c, d).wait_recv())
        if c == 0:
            load_left.wait()
            load_right.wait()

        def body(i, carry):
            at = pl.ds(pl.multiple_of(i * tile, tile), tile)
            product = jnp.dot(lefts[at, :], block_in[c], preferred_element_type=F32).astype(BF16)
            part = jnp.dot(product, rights[c * width : (c + 1) * width, :], preferred_element_type=F32)
            if c > 0:
                part = total[at, :] + part
            if c < chunks - 1:
                total[at, :] = part
            else:
                out = part.astype(BF16)
                wide = out.astype(F32)
                shampoo_sq[...] += jnp.sum((wide * wide).reshape(tile // 8, 8, size), axis=0)
                for e in range(chunks):
                    precond[e, at, :] = out[:, e * width : (e + 1) * width]
            return carry

        lax.fori_loop(0, size // tile, body, 0)

    for c in range(chunks + 2):
        if c >= 2:
            multiply(c - 2)
        if c < chunks:
            sum_and_send(c)

    lane = lax.broadcasted_iota(jnp.int32, (1, LANES), 1)
    mine = table[r, g, 0]
    mine_at = layer_of[r * rb + jnp.maximum(mine, 0)]
    used = jnp.where(mine >= 0, 1.0, 0.0).astype(F32)
    shampoo = jnp.where(lane == mine_at, used * jnp.sum(shampoo_sq[...], keepdims=True), 0.0)

    def layer_sum(j, carry):
        return carry + jnp.where(lane == layer_of[r * rb + j], jnp.sum(graft_sq[j], keepdims=True), 0.0)

    graft_total = lax.fori_loop(0, rb, layer_sum, jnp.zeros((1, LANES), F32))
    row = lax.broadcasted_iota(jnp.int32, (8, LANES), 0)
    stat = jnp.where(row == 0, graft_total, 0.0) + jnp.where(row == 1, shampoo, 0.0)
    stat_mine[...] = stat
    stat_group[g] = stat
    each_peer(lambda d: send_stat(d).start())
    for c in range(chunks):
        each_peer(lambda d: send_back(c, d).start())
    for c in range(chunks):
        rows_in[c][g] = precond[c, pl.ds(pl.multiple_of(g * rows, rows), rows), :]
    each_peer(lambda d: recv_stat(d).wait_recv())
    stat_rep[0] = jnp.sum(stat_group[...], axis=0)
    send_stat_rep(0, pair).start()
    send_stat_rep(0, pair).wait_recv()
    stat_rep[2] = stat_rep[0] + stat_rep[1]
    send_stat_rep(1, half).start()
    send_stat_rep(1, half).wait_recv()
    stat = stat_rep[2] + stat_rep[3]
    layer_scale = jnp.sqrt(stat[0:1]) * lax.rsqrt(stat[1:2] + 1e-06)

    def block_scale(j, carry):
        scale = jnp.sum(jnp.where(lane == layer_of[r * rb + j], layer_scale, 0.0), axis=1, keepdims=True)
        scales[j] = jnp.broadcast_to(step_rate * scale, (1, width))
        return carry

    lax.fori_loop(0, rb, block_scale, 0)

    def pass_on(c):
        send_other(c).wait_recv()
        send_core(c, 1).start()
        store_param(c, 1).start()

    for c in range(chunks):
        load_param(c).wait()
        each_peer(lambda d: recv_back(c, d).wait_recv())

        def update(j, carry):
            def find(d, at):
                return jnp.where(table[r, d, 0] == j, d, at)

            position = lax.fori_loop(0, n, find, 0)
            updated[c, j] = (param_in[c, j].astype(F32) - scales[j] * rows_in[c][position].astype(F32)).astype(BF16)
            return carry

        lax.fori_loop(0, rb, update, 0)
        send_other(c).start()
        send_core(c, 0).start()
        store_param(c, 0).start()
        if c > 0:
            pass_on(c - 1)
    pass_on(chunks - 1)

    for c in range(chunks):
        store_accum(c).wait()
        for which in range(2):
            store_param(c, which).wait()
            send_core(c, which).wait_send()
            recv_core(c, which).wait_recv()
            send_pair(c, which).wait_send()
        send_half(c).wait_send()
        send_other(c).wait_send()
        each_peer(lambda d: send_slot(c, d).wait_send())
        each_peer(lambda d: send_back(c, d).wait_send())
    each_peer(lambda d: send_stat(d).wait_send())
    send_stat_rep(0, pair).wait_send()
    send_stat_rep(1, half).wait_send()


CHUNKS = 4


def local(grad_parts, params, accum, left_pre, right_pre, slot_block, layer_of):
    n = lax.axis_size("group")
    assert lax.axis_size("rep") == 4 and left_pre.shape[2] == 1
    rb, rows, size = params.shape
    chunks = CHUNKS
    width = size // chunks
    tile = 256
    any_space = pl.BlockSpec(memory_space=pl.ANY)
    scalars = pl.BlockSpec(memory_space=pltpu.SMEM)
    dma = pltpu.SemaphoreType.DMA
    part = (chunks, rb, rows, width)
    twice = (chunks, 2, rb, rows, width)
    slots = (chunks, n, rows, width)
    whole = (chunks, size, width)
    vmem = pltpu.VMEM
    return pl.pallas_call(
        functools.partial(kernel, n, chunks, width, rb, rows, size, tile),
        out_shape=(
            jax.ShapeDtypeStruct((grad_parts.shape[1], rows, size), BF16),
            jax.ShapeDtypeStruct(accum.shape, F32),
        ),
        in_specs=[scalars] * 2 + [any_space] * 5,
        out_specs=(any_space, any_space),
        scratch_shapes=[
            vmem(twice, BF16), vmem(twice, BF16), vmem(part, BF16), vmem(part, BF16), vmem(part, BF16),
            vmem(slots, BF16), vmem(whole, BF16), vmem((size, size), BF16), vmem((size, size), BF16),
            vmem((size, size), F32), vmem(whole, BF16),
            [vmem(slots[1:], BF16)] * chunks, vmem(part, BF16), vmem(part, BF16), vmem(part, BF16), vmem(part, F32),
            vmem((rb, 8, width), F32), vmem((8, size), F32), vmem((rb, 1, width), F32),
            vmem((8, LANES), F32), vmem((n, 8, LANES), F32), vmem((4, 8, LANES), F32),
            dma((5, max(chunks, 2))), dma((chunks, 2)), dma((chunks, 2)), dma((chunks,)), dma((chunks,)),
            dma((chunks, n)), dma((chunks, n)), dma((chunks, n)), dma((chunks, n)),
            dma((n,)), dma((n,)), dma((2,)), dma((2,)), dma((chunks,)), dma((chunks,)),
            dma((chunks, 2)), dma((chunks, 2)), dma((3, chunks)),
        ],
        compiler_params=pltpu.CompilerParams(
            collective_id=0, has_side_effects=True, vmem_limit_bytes=60 * 1024 * 1024
        ),
    )(slot_block, layer_of, grad_parts, params, accum, left_pre, right_pre)


def solution(mesh):
    in_specs = (
        P("rep", None, "group", None),
        P("rep", "group", None),
        P("rep", "group", None),
        P("rep", "group", None, None, None),
        P("rep", "group", None, None, None),
        P(),
        P(),
    )
    out_specs = (P(None, "group", None), P("rep", "group", None))
    return jax.shard_map(local, mesh=mesh, in_specs=in_specs, out_specs=out_specs, check_vma=False)
```

```python
import functools

import jax
import jax.numpy as jnp
from jax import lax
from jax.experimental import pallas as pl
from jax.experimental.pallas import tpu as pltpu
from jax.sharding import PartitionSpec as P

MESH = pl.DeviceIdType.MESH
LAYERS = 8
LANES = 128
step_rate = 0.5
F32 = jnp.float32
BF16 = jnp.bfloat16


def kernel(
    n, chunks, width, rb, rows, size, tile,
    table_in, layer_in, grad, params, accum, left, right,
    new_params, new_accum,
    own, pair_in, half_out, half_in, summed, slot_out, block_in, lefts, rights, total, precond,
    rows_in, param_in, updated, other_in, acc, graft_sq, shampoo_sq, scales, stat_mine, stat_group, stat_rep,
    load_sem, pair_send, pair_recv, half_send, half_recv, slot_send, slot_recv, back_send, back_recv,
    stat_send, stat_recv, stat_rep_send, stat_rep_recv, other_send, other_recv, core_send, core_recv,
    store_sem, table, layer_of,
):
    g = lax.axis_index("group")
    r = lax.axis_index("rep")
    pair = r + 1 - 2 * (r % 2)
    half = r + 2 - 4 * ((r // 2) % 2)
    pair_half = pair + 2 - 4 * ((pair // 2) % 2)

    def cols(c):
        return pl.ds(c * width, width)

    def blocks(q):
        return pl.ds(q * rb, rb)

    def peer(k):
        return (g + 1 + (n // 2 - 1 + k) % (n - 1)) % n

    def remote(src, dst, send, recv, where):
        return pltpu.make_async_remote_copy(
            src_ref=src, dst_ref=dst, send_sem=send, recv_sem=recv, device_id=where, device_id_type=MESH
        )

    def load_own(c, which):
        q = (r, half)[which]
        return pltpu.make_async_copy(grad.at[0, blocks(q), :, cols(c)], own.at[c, which], load_sem.at[which, c])

    def load_accum(c):
        return pltpu.make_async_copy(accum.at[:, :, cols(c)], acc.at[c], load_sem.at[2, c])

    def load_param(c):
        return pltpu.make_async_copy(params.at[:, :, cols(c)], param_in.at[c], load_sem.at[3, c])

    load_table = pltpu.make_async_copy(table_in, table, load_sem.at[0, chunks])
    load_layers = pltpu.make_async_copy(layer_in, layer_of, load_sem.at[1, chunks])
    load_left = pltpu.make_async_copy(left.at[0, 0, 0], lefts, load_sem.at[4, 0])
    load_right = pltpu.make_async_copy(right.at[0, 0, 0], rights, load_sem.at[4, 1])

    def store_accum(c):
        return pltpu.make_async_copy(acc.at[c], new_accum.at[:, :, cols(c)], store_sem.at[0, c])

    def send_pair(c, which):
        q = (pair, pair_half)[which]
        return remote(
            grad.at[0, blocks(q), :, cols(c)], pair_in.at[c, which],
            pair_send.at[c, which], pair_recv.at[c, which], {"rep": pair},
        )

    def send_half(c):
        return remote(half_out.at[c], half_in.at[c], half_send.at[c], half_recv.at[c], {"rep": half})

    def send_slot(c, d):
        return remote(
            slot_out.at[c, d], block_in.at[c, pl.ds(g * rows, rows), :],
            slot_send.at[c, d], slot_recv.at[c, g], {"group": d},
        )

    def recv_slot(c, d):
        return remote(
            slot_out.at[c, d], block_in.at[c, pl.ds(d * rows, rows), :],
            slot_send.at[c, d], slot_recv.at[c, d], {"group": d},
        )

    def send_back(c, d):
        return remote(
            precond.at[c, pl.ds(d * rows, rows), :], rows_in[c].at[g],
            back_send.at[c, d], back_recv.at[c, g], {"group": d},
        )

    def recv_back(c, d):
        return remote(
            precond.at[c, pl.ds(d * rows, rows), :], rows_in[c].at[d],
            back_send.at[c, d], back_recv.at[c, d], {"group": d},
        )

    def send_stat(d):
        return remote(stat_mine, stat_group.at[g], stat_send.at[d], stat_recv.at[g], {"group": d})

    def recv_stat(d):
        return remote(stat_mine, stat_group.at[d], stat_send.at[d], stat_recv.at[d], {"group": d})

    def send_stat_rep(i, where):
        return remote(
            stat_rep.at[2 * i], stat_rep.at[2 * i + 1], stat_rep_send.at[i], stat_rep_recv.at[i], {"rep": where}
        )

    def send_other(c):
        return remote(updated.at[c], other_in.at[c], other_send.at[c], other_recv.at[c], {"rep": half})

    def send_core(c, which):
        src = (updated, other_in)[which]
        q = (r, half)[which]
        return remote(
            src.at[c], new_params.at[blocks(q), :, cols(c)],
            core_send.at[c, which], core_recv.at[c, which], {"rep": pair},
        )

    def recv_core(c, which):
        src = (updated, other_in)[which]
        q = (pair, pair_half)[which]
        return remote(
            src.at[c], new_params.at[blocks(q), :, cols(c)],
            core_send.at[c, which], core_recv.at[c, which], {"rep": pair},
        )

    def store_param(c, which):
        src = (updated, other_in)[which]
        q = (r, half)[which]
        return pltpu.make_async_copy(src.at[c], new_params.at[blocks(q), :, cols(c)], store_sem.at[1 + which, c])

    def each_peer(act):
        def body(k, carry):
            act(peer(k))
            return carry

        lax.fori_loop(0, n - 1, body, 0)

    for c in range(chunks):
        load_own(c, 1).start()
        load_own(c, 0).start()

    load_table.start()
    load_layers.start()
    barrier = pltpu.get_barrier_semaphore()
    each_peer(
        lambda d: pl.semaphore_signal(barrier, inc=1, device_id={"group": d}, device_id_type=MESH)
    )
    pl.semaphore_signal(barrier, inc=1, device_id={"rep": pair}, device_id_type=MESH)
    pl.semaphore_signal(barrier, inc=1, device_id={"rep": half}, device_id_type=MESH)
    pl.semaphore_wait(barrier, n + 1)

    for c in range(chunks):
        send_pair(c, 1).start()
        send_pair(c, 0).start()
    for c in range(chunks):
        load_accum(c).start()
    load_left.start()
    load_right.start()
    for c in range(chunks):
        load_param(c).start()

    load_table.wait()
    load_layers.wait()
    graft_sq[...] = jnp.zeros_like(graft_sq)
    shampoo_sq[...] = jnp.zeros_like(shampoo_sq)

    for c in range(chunks):
        load_own(c, 1).wait()
        send_pair(c, 1).wait_recv()

        def add_pair(j, carry):
            half_out[c, j] = (own[c, 1, j].astype(F32) + pair_in[c, 1, j].astype(F32)).astype(BF16)
            return carry

        lax.fori_loop(0, rb, add_pair, 0)
        send_half(c).start()

    def sum_and_send(c):
        load_own(c, 0).wait()
        send_pair(c, 0).wait_recv()
        send_half(c).wait_recv()

        def add_half(j, carry):
            summed[c, j] = (
                own[c, 0, j].astype(F32) + pair_in[c, 0, j].astype(F32) + half_in[c, j].astype(F32)
            ).astype(BF16)
            return carry

        lax.fori_loop(0, rb, add_half, 0)

        def fill(d, carry):
            slot_out[c, d] = summed[c, jnp.maximum(table[r, 0, d], 0)]
            return carry

        lax.fori_loop(0, n, fill, 0)
        each_peer(lambda d: send_slot(c, d).start())
        block_in[c, pl.ds(g * rows, rows), :] = slot_out[c, g]

        load_accum(c).wait()

        def graft(j, carry):
            gradient = summed[c, j].astype(F32)
            now = acc[c, j] + gradient * gradient
            acc[c, j] = now
            scaled = gradient * lax.rsqrt(now)
            graft_sq[j] += jnp.sum((scaled * scaled).reshape(rows // 8, 8, width), axis=0)
            return carry

        lax.fori_loop(0, rb, graft, 0)
        store_accum(c).start()

    def multiply(c):
        each_peer(lambda d: recv_slot(c, d).wait_recv())
        if c == 0:
            load_left.wait()
            load_right.wait()

        def body(i, carry):
            at = pl.ds(pl.multiple_of(i * tile, tile), tile)
            product = jnp.dot(lefts[at, :], block_in[c], preferred_element_type=F32).astype(BF16)
            part = jnp.dot(product, rights[c * width : (c + 1) * width, :], preferred_element_type=F32)
            if c > 0:
                part = total[at, :] + part
            if c < chunks - 1:
                total[at, :] = part
            else:
                out = part.astype(BF16)
                wide = out.astype(F32)
                shampoo_sq[...] += jnp.sum((wide * wide).reshape(tile // 8, 8, size), axis=0)
                for e in range(chunks):
                    precond[e, at, :] = out[:, e * width : (e + 1) * width]
            return carry

        lax.fori_loop(0, size // tile, body, 0)

    for c in range(chunks + 2):
        if c >= 2:
            multiply(c - 2)
        if c < chunks:
            sum_and_send(c)

    lane = lax.broadcasted_iota(jnp.int32, (1, LANES), 1)
    mine = table[r, 0, g]
    mine_at = layer_of[r * rb + jnp.maximum(mine, 0)]
    used = jnp.where(mine >= 0, 1.0, 0.0).astype(F32)
    shampoo = jnp.where(lane == mine_at, used * jnp.sum(shampoo_sq[...], keepdims=True), 0.0)

    def layer_sum(j, carry):
        return carry + jnp.where(lane == layer_of[r * rb + j], jnp.sum(graft_sq[j], keepdims=True), 0.0)

    graft_total = lax.fori_loop(0, rb, layer_sum, jnp.zeros((1, LANES), F32))
    row = lax.broadcasted_iota(jnp.int32, (8, LANES), 0)
    stat = jnp.where(row == 0, graft_total, 0.0) + jnp.where(row == 1, shampoo, 0.0)
    stat_mine[...] = stat
    stat_group[g] = stat
    each_peer(lambda d: send_stat(d).start())
    for c in range(chunks):
        each_peer(lambda d: send_back(c, d).start())
    for c in range(chunks):
        rows_in[c][g] = precond[c, pl.ds(pl.multiple_of(g * rows, rows), rows), :]
    each_peer(lambda d: recv_stat(d).wait_recv())
    stat_rep[0] = jnp.sum(stat_group[...], axis=0)
    send_stat_rep(0, pair).start()
    send_stat_rep(0, pair).wait_recv()
    stat_rep[2] = stat_rep[0] + stat_rep[1]
    send_stat_rep(1, half).start()
    send_stat_rep(1, half).wait_recv()
    stat = stat_rep[2] + stat_rep[3]
    layer_scale = jnp.sqrt(stat[0:1]) * lax.rsqrt(stat[1:2] + 1e-06)

    def block_scale(j, carry):
        scale = jnp.sum(jnp.where(lane == layer_of[r * rb + j], layer_scale, 0.0), axis=1, keepdims=True)
        scales[j] = jnp.broadcast_to(step_rate * scale, (1, width))
        return carry

    lax.fori_loop(0, rb, block_scale, 0)

    def pass_on(c):
        send_other(c).wait_recv()
        send_core(c, 1).start()
        store_param(c, 1).start()

    for c in range(chunks):
        load_param(c).wait()
        each_peer(lambda d: recv_back(c, d).wait_recv())

        def update(j, carry):
            def find(d, at):
                return jnp.where(table[r, 0, d] == j, d, at)

            position = lax.fori_loop(0, n, find, 0)
            updated[c, j] = (param_in[c, j].astype(F32) - scales[j] * rows_in[c][position].astype(F32)).astype(BF16)
            return carry

        lax.fori_loop(0, rb, update, 0)
        send_other(c).start()
        send_core(c, 0).start()
        store_param(c, 0).start()
        if c > 0:
            pass_on(c - 1)
    pass_on(chunks - 1)

    for c in range(chunks):
        store_accum(c).wait()
        for which in range(2):
            store_param(c, which).wait()
            send_core(c, which).wait_send()
            recv_core(c, which).wait_recv()
            send_pair(c, which).wait_send()
        send_half(c).wait_send()
        send_other(c).wait_send()
        each_peer(lambda d: send_slot(c, d).wait_send())
        each_peer(lambda d: send_back(c, d).wait_send())
    each_peer(lambda d: send_stat(d).wait_send())
    send_stat_rep(0, pair).wait_send()
    send_stat_rep(1, half).wait_send()


CHUNKS = 8


def local(grad_parts, params, accum, left_pre, right_pre, slot_block, layer_of):
    n = lax.axis_size("group")
    assert lax.axis_size("rep") == 4 and left_pre.shape[2] == 1
    rb, rows, size = params.shape
    chunks = CHUNKS
    width = size // chunks
    tile = 256
    any_space = pl.BlockSpec(memory_space=pl.ANY)
    dma = pltpu.SemaphoreType.DMA
    part = (chunks, rb, rows, width)
    twice = (chunks, 2, rb, rows, width)
    slots = (chunks, n, rows, width)
    whole = (chunks, size, width)
    vmem = pltpu.VMEM
    operands = (jnp.swapaxes(slot_block, 1, 2), layer_of, grad_parts, params, accum, left_pre, right_pre)
    operands = [pltpu.with_memory_space_constraint(x, pltpu.HBM) for x in operands]
    return pl.pallas_call(
        functools.partial(kernel, n, chunks, width, rb, rows, size, tile),
        out_shape=(
            jax.ShapeDtypeStruct((grad_parts.shape[1], rows, size), BF16),
            jax.ShapeDtypeStruct(accum.shape, F32),
        ),
        in_specs=[pl.BlockSpec(memory_space=pltpu.HBM)] * 7,
        out_specs=(any_space, any_space),
        scratch_shapes=[
            vmem(twice, BF16), vmem(twice, BF16), vmem(part, BF16), vmem(part, BF16), vmem(part, BF16),
            vmem(slots, BF16), vmem(whole, BF16), vmem((size, size), BF16), vmem((size, size), BF16),
            vmem((size, size), F32), vmem(whole, BF16),
            [vmem(slots[1:], BF16)] * chunks, vmem(part, BF16), vmem(part, BF16), vmem(part, BF16), vmem(part, F32),
            vmem((rb, 8, width), F32), vmem((8, size), F32), vmem((rb, 1, width), F32),
            vmem((8, LANES), F32), vmem((n, 8, LANES), F32), vmem((4, 8, LANES), F32),
            dma((5, chunks + 1)), dma((chunks, 2)), dma((chunks, 2)), dma((chunks,)), dma((chunks,)),
            dma((chunks, n)), dma((chunks, n)), dma((chunks, n)), dma((chunks, n)),
            dma((n,)), dma((n,)), dma((2,)), dma((2,)), dma((chunks,)), dma((chunks,)),
            dma((chunks, 2)), dma((chunks, 2)), dma((3, chunks)),
            pltpu.SMEM((slot_block.shape[0], 1, n), jnp.int32), pltpu.SMEM(layer_of.shape, jnp.int32),
        ],
        compiler_params=pltpu.CompilerParams(
            collective_id=0, has_side_effects=True, vmem_limit_bytes=38 * 1024 * 1024
        ),
    )(*operands)


def solution(mesh):
    in_specs = (
        P("rep", None, "group", None),
        P("rep", "group", None),
        P("rep", "group", None),
        P("rep", "group", None, None, None),
        P("rep", "group", None, None, None),
        P(),
        P(),
    )
    out_specs = (P(None, "group", None), P("rep", "group", None))
    return jax.shard_map(local, mesh=mesh, in_specs=in_specs, out_specs=out_specs, check_vma=False)
```

```python
import functools

import jax
import jax.numpy as jnp
from jax import lax
from jax.experimental import pallas as pl
from jax.experimental.pallas import tpu as pltpu
from jax.sharding import PartitionSpec as P

MESH = pl.DeviceIdType.MESH
LAYERS = 8
LANES = 128
step_rate = 0.5
F32 = jnp.float32
BF16 = jnp.bfloat16


def kernel(
    n, chunks, width, rb, rows, size, tile,
    table_in, layer_in, grad, params, accum, left, right,
    new_params, new_accum,
    own, pair_in, half_out, half_in, summed, slot_out, block_in, lefts, rights, total, precond,
    rows_in, param_in, updated, other_in, acc, graft_sq, shampoo_sq, scales, stat_mine, stat_group, stat_rep,
    load_sem, pair_send, pair_recv, half_send, half_recv, slot_send, slot_recv, back_send, back_recv,
    stat_send, stat_recv, stat_rep_send, stat_rep_recv, other_send, other_recv, core_send, core_recv,
    store_sem, table, layer_of,
):
    g = lax.axis_index("group")
    r = lax.axis_index("rep")
    pair = r + 1 - 2 * (r % 2)
    half = r + 2 - 4 * ((r // 2) % 2)
    pair_half = pair + 2 - 4 * ((pair // 2) % 2)

    part = rows // 2
    ahead = ((0, 0, part), (0, part, part)) + tuple((c, 0, rows) for c in range(1, chunks))
    final = chunks - 1
    behind = tuple((c, 0, rows) for c in range(final)) + ((final, 0, part), (final, part, part))
    pieces = chunks + 1

    def cols(c):
        return pl.ds(c * width, width)

    def blocks(q):
        return pl.ds(q * rb, rb)

    def peer(k):
        return (g + 1 + (n // 2 - 1 + k) % (n - 1)) % n

    def remote(src, dst, send, recv, where):
        return pltpu.make_async_remote_copy(
            src_ref=src, dst_ref=dst, send_sem=send, recv_sem=recv, device_id=where, device_id_type=MESH
        )

    def load_own(c, which):
        q = (r, half)[which]
        return pltpu.make_async_copy(grad.at[0, blocks(q), :, cols(c)], own.at[c, which], load_sem.at[which, c])

    def load_accum(c):
        return pltpu.make_async_copy(accum.at[:, :, cols(c)], acc.at[c], load_sem.at[2, c])

    def load_param(c):
        return pltpu.make_async_copy(params.at[:, :, cols(c)], param_in.at[c], load_sem.at[3, c])

    load_table = pltpu.make_async_copy(table_in, table, load_sem.at[0, chunks])
    load_layers = pltpu.make_async_copy(layer_in, layer_of, load_sem.at[1, chunks])
    load_left = pltpu.make_async_copy(left.at[0, 0, 0], lefts, load_sem.at[4, 0])
    load_right = pltpu.make_async_copy(right.at[0, 0, 0], rights, load_sem.at[4, 1])

    def store_accum(c):
        return pltpu.make_async_copy(acc.at[c], new_accum.at[:, :, cols(c)], store_sem.at[0, c])

    def send_pair(c, which):
        q = (pair, pair_half)[which]
        return remote(
            grad.at[0, blocks(q), :, cols(c)], pair_in.at[c, which],
            pair_send.at[c, which], pair_recv.at[c, which], {"rep": pair},
        )

    def send_half(p):
        c, a, m = ahead[p]
        return remote(
            half_out.at[c, :, pl.ds(a, m), :], half_in.at[c, :, pl.ds(a, m), :],
            half_send.at[p], half_recv.at[p], {"rep": half},
        )

    def slot(p, d, source):
        c, a, m = ahead[p]
        return remote(
            slot_out.at[c, d, pl.ds(a, m), :], block_in.at[c, pl.ds(source * rows + a, m), :],
            slot_send.at[p, d], slot_recv.at[p, source], {"group": d},
        )

    def send_slot(p, d):
        return slot(p, d, g)

    def recv_slot(p, d):
        return slot(p, d, d)

    def back(p, d, source):
        c, a, m = behind[p]
        return remote(
            precond.at[c, pl.ds(d * rows + a, m), :], rows_in[p].at[source],
            back_send.at[p, d], back_recv.at[p, source], {"group": d},
        )

    def send_back(p, d):
        return back(p, d, g)

    def recv_back(p, d):
        return back(p, d, d)

    def send_stat(d):
        return remote(stat_mine, stat_group.at[g], stat_send.at[d], stat_recv.at[g], {"group": d})

    def recv_stat(d):
        return remote(stat_mine, stat_group.at[d], stat_send.at[d], stat_recv.at[d], {"group": d})

    def send_stat_rep(i, where):
        return remote(
            stat_rep.at[2 * i], stat_rep.at[2 * i + 1], stat_rep_send.at[i], stat_rep_recv.at[i], {"rep": where}
        )

    def send_other(p):
        c, a, m = behind[p]
        return remote(
            updated.at[c, :, pl.ds(a, m), :], other_in.at[c, :, pl.ds(a, m), :],
            other_send.at[p], other_recv.at[p], {"rep": half},
        )

    def result(p, which, q):
        c, a, m = behind[p]
        src = (updated, other_in)[which]
        return src.at[c, :, pl.ds(a, m), :], new_params.at[blocks(q), pl.ds(a, m), cols(c)]

    def send_core(p, which):
        src, dst = result(p, which, (r, half)[which])
        return remote(src, dst, core_send.at[p, which], core_recv.at[p, which], {"rep": pair})

    def recv_core(p, which):
        src, dst = result(p, which, (pair, pair_half)[which])
        return remote(src, dst, core_send.at[p, which], core_recv.at[p, which], {"rep": pair})

    def store_param(p, which):
        src, dst = result(p, which, (r, half)[which])
        return pltpu.make_async_copy(src, dst, store_sem.at[1 + which, p])

    def each_peer(act):
        def body(k, carry):
            act(peer(k))
            return carry

        lax.fori_loop(0, n - 1, body, 0)

    for c in range(chunks):
        load_own(c, 1).start()
        load_own(c, 0).start()

    load_table.start()
    load_layers.start()
    barrier = pltpu.get_barrier_semaphore()
    each_peer(
        lambda d: pl.semaphore_signal(barrier, inc=1, device_id={"group": d}, device_id_type=MESH)
    )
    pl.semaphore_signal(barrier, inc=1, device_id={"rep": pair}, device_id_type=MESH)
    pl.semaphore_signal(barrier, inc=1, device_id={"rep": half}, device_id_type=MESH)
    pl.semaphore_wait(barrier, n + 1)

    for c in range(chunks):
        send_pair(c, 1).start()
        send_pair(c, 0).start()
    for c in range(chunks):
        load_accum(c).start()
    load_left.start()
    load_right.start()
    for c in range(chunks):
        load_param(c).start()

    load_table.wait()
    load_layers.wait()
    graft_sq[...] = jnp.zeros_like(graft_sq)
    shampoo_sq[...] = jnp.zeros_like(shampoo_sq)

    for c in range(chunks):
        load_own(c, 1).wait()
        send_pair(c, 1).wait_recv()

        def add_pair(j, carry):
            half_out[c, j] = (own[c, 1, j].astype(F32) + pair_in[c, 1, j].astype(F32)).astype(BF16)
            return carry

        lax.fori_loop(0, rb, add_pair, 0)
        for p in range(pieces):
            if ahead[p][0] == c:
                send_half(p).start()

    def sum_and_send(p):
        c, a, m = ahead[p]
        at = pl.ds(a, m)
        if a == 0:
            load_own(c, 0).wait()
            send_pair(c, 0).wait_recv()
        send_half(p).wait_recv()

        def add_half(j, carry):
            summed[c, j, at, :] = (
                own[c, 0, j, at, :].astype(F32) + pair_in[c, 0, j, at, :].astype(F32) + half_in[c, j, at, :].astype(F32)
            ).astype(BF16)
            return carry

        lax.fori_loop(0, rb, add_half, 0)

        def fill(d, carry):
            slot_out[c, d, at, :] = summed[c, jnp.maximum(table[r, 0, d], 0), at, :]
            return carry

        lax.fori_loop(0, n, fill, 0)
        each_peer(lambda d: send_slot(p, d).start())
        block_in[c, pl.ds(pl.multiple_of(g * rows + a, m), m), :] = slot_out[c, g, at, :]

        if a == 0:
            load_accum(c).wait()

        def graft(j, carry):
            gradient = summed[c, j, at, :].astype(F32)
            now = acc[c, j, at, :] + gradient * gradient
            acc[c, j, at, :] = now
            scaled = gradient * lax.rsqrt(now)
            graft_sq[j] += jnp.sum((scaled * scaled).reshape(m // 8, 8, width), axis=0)
            return carry

        lax.fori_loop(0, rb, graft, 0)
        if a + m == rows:
            store_accum(c).start()

    def multiply(c):
        for p in range(pieces):
            if ahead[p][0] == c:
                each_peer(lambda d: recv_slot(p, d).wait_recv())
        if c == 0:
            load_left.wait()
            load_right.wait()

        tiles = size // tile
        first = (g * rows) // tile + tiles // 2

        def body(step, carry):
            i = (first + step) % tiles
            at = pl.ds(pl.multiple_of(i * tile, tile), tile)
            product = jnp.dot(lefts[at, :], block_in[c], preferred_element_type=F32).astype(BF16)
            part = jnp.dot(product, rights[c * width : (c + 1) * width, :], preferred_element_type=F32)
            if c > 0:
                part = total[at, :] + part
            if c < chunks - 1:
                total[at, :] = part
            else:
                out = part.astype(BF16)
                wide = out.astype(F32)
                shampoo_sq[...] += jnp.sum((wide * wide).reshape(tile // 8, 8, size), axis=0)
                for e in range(chunks):
                    precond[e, at, :] = out[:, e * width : (e + 1) * width]

                def send_tile(k, carry):
                    d = i * (tile // rows) + k

                    @pl.when(d != g)
                    def _():
                        send_back(0, d).start()

                    return carry

                lax.fori_loop(0, tile // rows, send_tile, 0)
            return carry

        lax.fori_loop(0, tiles, body, 0)

    for p in range(chunks + LAG):
        if p >= LAG:
            multiply(p - LAG)
        if p < pieces:
            sum_and_send(p)

    lane = lax.broadcasted_iota(jnp.int32, (1, LANES), 1)
    mine = table[r, 0, g]
    mine_at = layer_of[r * rb + jnp.maximum(mine, 0)]
    used = jnp.where(mine >= 0, 1.0, 0.0).astype(F32)
    shampoo = jnp.where(lane == mine_at, used * jnp.sum(shampoo_sq[...], keepdims=True), 0.0)

    def layer_sum(j, carry):
        return carry + jnp.where(lane == layer_of[r * rb + j], jnp.sum(graft_sq[j], keepdims=True), 0.0)

    graft_total = lax.fori_loop(0, rb, layer_sum, jnp.zeros((1, LANES), F32))
    row = lax.broadcasted_iota(jnp.int32, (8, LANES), 0)
    stat = jnp.where(row == 0, graft_total, 0.0) + jnp.where(row == 1, shampoo, 0.0)
    stat_mine[...] = stat
    stat_group[g] = stat
    each_peer(lambda d: send_stat(d).start())
    for p in range(1, pieces):
        each_peer(lambda d: send_back(p, d).start())
    for p in range(pieces):
        c, a, m = behind[p]
        rows_in[p][g] = precond[c, pl.ds(pl.multiple_of(g * rows + a, m), m), :]
    each_peer(lambda d: recv_stat(d).wait_recv())
    stat_rep[0] = jnp.sum(stat_group[...], axis=0)
    send_stat_rep(0, pair).start()
    send_stat_rep(0, pair).wait_recv()
    stat_rep[2] = stat_rep[0] + stat_rep[1]
    send_stat_rep(1, half).start()
    send_stat_rep(1, half).wait_recv()
    stat = stat_rep[2] + stat_rep[3]
    layer_scale = jnp.sqrt(stat[0:1]) * lax.rsqrt(stat[1:2] + 1e-06)

    def block_scale(j, carry):
        scale = jnp.sum(jnp.where(lane == layer_of[r * rb + j], layer_scale, 0.0), axis=1, keepdims=True)
        scales[j] = jnp.broadcast_to(step_rate * scale, (1, width))
        return carry

    lax.fori_loop(0, rb, block_scale, 0)

    def pass_on(p):
        send_other(p).wait_recv()
        send_core(p, 1).start()
        store_param(p, 1).start()

    for p in range(pieces):
        c, a, m = behind[p]
        at = pl.ds(a, m)
        if a == 0:
            load_param(c).wait()
        each_peer(lambda d: recv_back(p, d).wait_recv())

        def update(j, carry):
            def find(d, found):
                return jnp.where(table[r, 0, d] == j, d, found)

            position = lax.fori_loop(0, n, find, 0)
            updated[c, j, at, :] = (
                param_in[c, j, at, :].astype(F32) - scales[j] * rows_in[p][position].astype(F32)
            ).astype(BF16)
            return carry

        lax.fori_loop(0, rb, update, 0)
        send_other(p).start()
        send_core(p, 0).start()
        store_param(p, 0).start()
        if p > 0:
            pass_on(p - 1)
    pass_on(pieces - 1)

    for c in range(chunks):
        store_accum(c).wait()
        for which in range(2):
            send_pair(c, which).wait_send()
    for p in range(pieces):
        for which in range(2):
            store_param(p, which).wait()
            send_core(p, which).wait_send()
            recv_core(p, which).wait_recv()
        send_half(p).wait_send()
        send_other(p).wait_send()
        each_peer(lambda d: send_slot(p, d).wait_send())
        each_peer(lambda d: send_back(p, d).wait_send())
    each_peer(lambda d: send_stat(d).wait_send())
    send_stat_rep(0, pair).wait_send()
    send_stat_rep(1, half).wait_send()


CHUNKS = 8
LAG = 4


def local(grad_parts, params, accum, left_pre, right_pre, slot_block, layer_of):
    n = lax.axis_size("group")
    assert lax.axis_size("rep") == 4 and left_pre.shape[2] == 1
    rb, rows, size = params.shape
    chunks = CHUNKS
    more = chunks + 1
    width = size // chunks
    tile = 256
    any_space = pl.BlockSpec(memory_space=pl.ANY)
    dma = pltpu.SemaphoreType.DMA
    part = (chunks, rb, rows, width)
    twice = (chunks, 2, rb, rows, width)
    slots = (chunks, n, rows, width)
    whole = (chunks, size, width)
    vmem = pltpu.VMEM
    operands = (jnp.swapaxes(slot_block, 1, 2), layer_of, grad_parts, params, accum, left_pre, right_pre)
    operands = [pltpu.with_memory_space_constraint(x, pltpu.HBM) for x in operands]
    return pl.pallas_call(
        functools.partial(kernel, n, chunks, width, rb, rows, size, tile),
        out_shape=(
            jax.ShapeDtypeStruct((grad_parts.shape[1], rows, size), BF16),
            jax.ShapeDtypeStruct(accum.shape, F32),
        ),
        in_specs=[pl.BlockSpec(memory_space=pltpu.HBM)] * 7,
        out_specs=(any_space, any_space),
        scratch_shapes=[
            vmem(twice, BF16), vmem(twice, BF16), vmem(part, BF16), vmem(part, BF16), vmem(part, BF16),
            vmem(slots, BF16), vmem(whole, BF16), vmem((size, size), BF16), vmem((size, size), BF16),
            vmem((size, size), F32), vmem(whole, BF16),
            [vmem((n, m, width), BF16) for m in [rows] * (chunks - 1) + [rows // 2] * 2], vmem(part, BF16), vmem(part, BF16), vmem(part, BF16), vmem(part, F32),
            vmem((rb, 8, width), F32), vmem((8, size), F32), vmem((rb, 1, width), F32),
            vmem((8, LANES), F32), vmem((n, 8, LANES), F32), vmem((4, 8, LANES), F32),
            dma((5, more)), dma((chunks, 2)), dma((chunks, 2)), dma((more,)), dma((more,)),
            dma((more, n)), dma((more, n)), dma((more, n)), dma((more, n)),
            dma((n,)), dma((n,)), dma((2,)), dma((2,)), dma((more,)), dma((more,)),
            dma((more, 2)), dma((more, 2)), dma((3, more)),
            pltpu.SMEM((slot_block.shape[0], 1, n), jnp.int32), pltpu.SMEM(layer_of.shape, jnp.int32),
        ],
        compiler_params=pltpu.CompilerParams(
            collective_id=0, has_side_effects=True, vmem_limit_bytes=38 * 1024 * 1024
        ),
    )(*operands)


def solution(mesh):
    in_specs = (
        P("rep", None, "group", None),
        P("rep", "group", None),
        P("rep", "group", None),
        P("rep", "group", None, None, None),
        P("rep", "group", None, None, None),
        P(),
        P(),
    )
    out_specs = (P(None, "group", None), P("rep", "group", None))
    return jax.shard_map(local, mesh=mesh, in_specs=in_specs, out_specs=out_specs, check_vma=False)
```
